32 devices in a mesh: dp: 1 (over z), tp: 4 (over y), ep: 8 (over x, core).
Axes of the slice: x: 4, y: 4, z: 1, core: 2. Of those that a mesh axis runs over, the one named last changes fastest.
The devices are a block of a 4x4x8 slice.
Arguments:
- hidden: bfloat16 [256, 2048], P(('dp', 'ep'))
- seq_lens: int32 [256], P(('dp', 'ep'))
- rope_cos: float32 [256, 64], P(('dp', 'ep'))
- rope_sin: float32 [256, 64], P(('dp', 'ep'))
- ln1_scale: bfloat16 [2048], replicated
- ln1_bias: bfloat16 [2048], replicated
- w_qkv: bfloat16 [2048, 5120], P(None, 'tp')
- b_qkv: bfloat16 [5120], P('tp')
- w_out: bfloat16 [4096, 2048], P('tp')
- b_out: bfloat16 [2048], replicated
- k_cache: bfloat16 [256, 256, 4, 128], P(('dp', 'ep'), None, 'tp')
- v_cache: bfloat16 [256, 256, 4, 128], P(('dp', 'ep'), None, 'tp')
- ln2_scale: bfloat16 [2048], replicated
- ln2_bias: bfloat16 [2048], replicated
- w_router: bfloat16 [2048, 128], replicated
- expert_ids: int32 [256, 8], P(('dp', 'ep'))
- w_gate: bfloat16 [128, 2048, 768], P('ep', None, 'tp')
- w_up: bfloat16 [128, 2048, 768], P('ep', None, 'tp')
- w_down: bfloat16 [128, 768, 2048], P('ep', 'tp')
Outputs:
- output 1: bfloat16 [256, 2048], P(('dp', 'ep'))
- output 2: bfloat16 [256, 256, 4, 128], P(('dp', 'ep'), None, 'tp')
- output 3: bfloat16 [256, 256, 4, 128], P(('dp', 'ep'), None, 'tp')
All inputs are finite; a program needn't handle non-finite values.
Results may differ from the reference program's by a relative error of at most 0.0117888.
Values are sent between devices in bfloat16 or wider.
A program may use at most 768 MiB of HBM per device.

```python
import jax
import jax.numpy as jnp
from jax import lax

D = 2048
HEADS = 32
KV_HEADS = 4
HEAD = 128
EXPERTS = 128
TOP = 8
FF = 768
BATCH = 32
SMAX = 256
EP_SHARDS = 8

TOKENS = EP_SHARDS * BATCH
Q_PER_GROUP = HEADS // KV_HEADS
QKV_COLS = KV_HEADS * (Q_PER_GROUP + 2) * HEAD
CAP = (2 * TOP * BATCH + EXPERTS - 1) // EXPERTS
EPS = 1e-5
ROPE_BASE = 10000.0


def gaussian(one_key, out_shape):
    return jax.random.normal(one_key, out_shape, jnp.float32)


def draw_routing(route_key):
    hot_key, shard_key = jax.random.split(route_key)
    hot_order = jax.random.permutation(hot_key, EXPERTS)
    n_pairs = TOP * BATCH
    even_total = n_pairs - n_pairs // 2
    even_rows = even_total // EXPERTS + (jnp.arange(EXPERTS) < even_total % EXPERTS).astype(jnp.int32)

    def one_shard(one_key):
        even_key, order_key = jax.random.split(one_key)
        even_order = jax.random.permutation(even_key, EXPERTS)
        counts = jnp.zeros((EXPERTS,), jnp.int32).at[even_order].set(even_rows)
        free_room = CAP - counts[hot_order]
        before = jnp.cumsum(free_room) - free_room
        extra_rows = jnp.minimum(jnp.maximum(n_pairs // 2 - before, 0), free_room)
        counts = counts.at[hot_order].add(extra_rows)
        run_ends = jnp.cumsum(counts)
        slot_expert = jnp.sum((jnp.arange(n_pairs)[:, None] >= run_ends[None, :]).astype(jnp.int32), axis=1)
        choices = slot_expert.reshape(TOP, BATCH).T
        return choices[jax.random.permutation(order_key, BATCH)]

    picked = jax.vmap(one_shard)(jax.random.split(shard_key, EP_SHARDS))
    return picked.reshape(TOKENS, TOP).astype(jnp.int32)


def draw_lengths(len_key):
    draw_key, mark_key = jax.random.split(len_key)
    lengths = jax.random.randint(draw_key, (TOKENS,), SMAX // 16, SMAX)
    mark_order = jax.random.permutation(mark_key, TOKENS)
    lengths = lengths.at[mark_order[0]].set(SMAX - 1).at[mark_order[1]].set(SMAX // 16)
    return lengths.astype(jnp.int32)


def draw_rope(rope_key, lengths, factor_min, factor_max):
    rescale = jax.random.uniform(rope_key, (HEAD // 2,), jnp.float32, factor_min, factor_max)
    inv_freq = ROPE_BASE ** (-jnp.arange(HEAD // 2, dtype=jnp.float32) * 2.0 / HEAD)
    angles = lengths.astype(jnp.float32)[:, None] * inv_freq[None, :] / rescale[None, :]
    return jnp.cos(angles), jnp.sin(angles)


def setup_inputs(seed: int = 0, part: int = 0) -> dict:
    shared_key = jax.random.key(seed)
    part_key = jax.random.fold_in(jax.random.key(seed + 1), part)
    weight_keys = jax.random.split(shared_key, 12)
    part_keys = jax.random.split(part_key, 7)
    bf16 = jnp.bfloat16
    lengths = draw_lengths(part_keys[0])
    rope_cos, rope_sin = draw_rope(part_keys[1], lengths, 1.0, 8.0)
    hidden = gaussian(part_keys[2], (TOKENS, D))
    k_cache = 2.0 * gaussian(part_keys[3], (TOKENS, SMAX, KV_HEADS, HEAD))
    v_cache = 0.5 * gaussian(part_keys[4], (TOKENS, 1, KV_HEADS, HEAD)) + gaussian(part_keys[5], (TOKENS, SMAX, KV_HEADS, HEAD))
    expert_ids = draw_routing(part_keys[6])
    return {
        'hidden': hidden.astype(bf16),
        'seq_lens': lengths,
        'rope_cos': rope_cos,
        'rope_sin': rope_sin,
        'ln1_scale': (1.0 + 0.3 * gaussian(weight_keys[0], (D,))).astype(bf16),
        'ln1_bias': (0.3 * gaussian(weight_keys[1], (D,))).astype(bf16),
        'w_qkv': (gaussian(weight_keys[2], (D, QKV_COLS)) * D ** -0.5).astype(bf16),
        'b_qkv': (0.5 * gaussian(weight_keys[3], (QKV_COLS,))).astype(bf16),
        'w_out': (gaussian(weight_keys[4], (HEADS * HEAD, D)) * (HEADS * HEAD) ** -0.5).astype(bf16),
        'b_out': (0.3 * gaussian(weight_keys[5], (D,))).astype(bf16),
        'k_cache': k_cache.astype(bf16),
        'v_cache': v_cache.astype(bf16),
        'ln2_scale': (1.0 + 0.3 * gaussian(weight_keys[6], (D,))).astype(bf16),
        'ln2_bias': (0.3 * gaussian(weight_keys[7], (D,))).astype(bf16),
        'w_router': (gaussian(weight_keys[8], (D, EXPERTS)) * D ** -0.5).astype(bf16),
        'expert_ids': expert_ids,
        'w_gate': (gaussian(weight_keys[9], (EXPERTS, D, FF)) * D ** -0.5).astype(bf16),
        'w_up': (gaussian(weight_keys[10], (EXPERTS, D, FF)) * D ** -0.5).astype(bf16),
        'w_down': (gaussian(weight_keys[11], (EXPERTS, FF, D)) * FF ** -0.5).astype(bf16),
    }


def layer_norm(values, ln_scale, ln_bias):
    vals_f32 = values.astype(jnp.float32)
    row_mean = jnp.mean(vals_f32, axis=-1, keepdims=True)
    centered = vals_f32 - row_mean
    row_var = jnp.mean(centered * centered, axis=-1, keepdims=True)
    normed = centered * lax.rsqrt(row_var + EPS)
    return (normed * ln_scale.astype(jnp.float32) + ln_bias.astype(jnp.float32)).astype(jnp.bfloat16)


def apply_rope(values, cos_part, sin_part):
    half_dim = values.shape[-1] // 2
    vals_f32 = values.astype(jnp.float32)
    first_half = vals_f32[..., :half_dim]
    second_half = vals_f32[..., half_dim:]
    rotated = jnp.concatenate([first_half * cos_part - second_half * sin_part, second_half * cos_part + first_half * sin_part], axis=-1)
    return rotated.astype(jnp.bfloat16)


def reference(hidden, seq_lens, rope_cos, rope_sin, ln1_scale, ln1_bias, w_qkv, b_qkv, w_out, b_out, k_cache, v_cache, ln2_scale, ln2_bias, w_router, expert_ids, w_gate, w_up, w_down):
    normed = layer_norm(hidden, ln1_scale, ln1_bias)
    qkv_rows = (jnp.dot(normed, w_qkv, preferred_element_type=jnp.float32) + b_qkv.astype(jnp.float32)).astype(jnp.bfloat16)
    qkv_rows = qkv_rows.reshape(TOKENS, KV_HEADS, Q_PER_GROUP + 2, HEAD)
    queries = apply_rope(qkv_rows[:, :, :Q_PER_GROUP], rope_cos[:, None, None, :], rope_sin[:, None, None, :])
    key_new = apply_rope(qkv_rows[:, :, Q_PER_GROUP], rope_cos[:, None, :], rope_sin[:, None, :])
    value_new = qkv_rows[:, :, Q_PER_GROUP + 1]
    positions = jnp.arange(SMAX)
    write_mask = (positions[None, :] == seq_lens[:, None])[:, :, None, None]
    k_cache_out = jnp.where(write_mask, key_new[:, None], k_cache)
    v_cache_out = jnp.where(write_mask, value_new[:, None], v_cache)

    def attend(per_seq):
        q_one, k_one, v_one, len_one = per_seq
        scores = jnp.einsum('gqh,sgh->gqs', q_one.astype(jnp.float32), k_one.astype(jnp.float32)) * HEAD ** -0.5
        scores = jnp.where(positions[None, None, :] <= len_one, scores, -jnp.inf)
        attn_probs = jax.nn.softmax(scores, axis=-1).astype(jnp.bfloat16)
        return jnp.einsum('gqs,sgh->gqh', attn_probs.astype(jnp.float32), v_one.astype(jnp.float32)).astype(jnp.bfloat16)

    context = lax.map(attend, (queries, k_cache_out, v_cache_out, seq_lens))
    attn_full = jnp.dot(context.reshape(TOKENS, HEADS * HEAD), w_out, preferred_element_type=jnp.float32)
    hidden_mid = (hidden.astype(jnp.float32) + attn_full + b_out.astype(jnp.float32)).astype(jnp.bfloat16)
    normed2 = layer_norm(hidden_mid, ln2_scale, ln2_bias)
    logits = jnp.dot(normed2, w_router, preferred_element_type=jnp.float32)
    chosen = jnp.take_along_axis(logits, expert_ids, axis=1)
    gate_probs = jax.nn.softmax(chosen, axis=-1).astype(jnp.bfloat16).astype(jnp.float32)
    mix_weights = jnp.sum(jax.nn.one_hot(expert_ids, EXPERTS, dtype=jnp.float32) * gate_probs[:, :, None], axis=1)

    def expert_step(moe_acc, per_expert):
        gate_w, up_w, down_w, weight = per_expert
        gate_pre = jnp.dot(normed2, gate_w, preferred_element_type=jnp.float32)
        up_pre = jnp.dot(normed2, up_w, preferred_element_type=jnp.float32)
        hidden_act = (jax.nn.silu(gate_pre) * up_pre).astype(jnp.bfloat16)
        expert_out = jnp.dot(hidden_act, down_w, preferred_element_type=jnp.float32).astype(jnp.bfloat16)
        return moe_acc + weight[:, None] * expert_out.astype(jnp.float32), None

    moe_sum, _ = lax.scan(expert_step, jnp.zeros((TOKENS, D), jnp.float32), (w_gate, w_up, w_down, mix_weights.T))
    hidden_out = (hidden_mid.astype(jnp.float32) + moe_sum).astype(jnp.bfloat16)
    return (hidden_out, k_cache_out, v_cache_out)
```

```python
import functools

import jax
import jax.numpy as jnp
from jax import lax
from jax.experimental import pallas as pl
from jax.experimental.pallas import tpu as pltpu
from jax.sharding import PartitionSpec as P

EPS = 1e-5
F32 = jnp.float32
BF16 = jnp.bfloat16
MESH = pl.DeviceIdType.MESH
NT = (((1,), (1,)), ((), ()))


def row_norm(vals_f32, ln_scale, ln_bias):
    row_mean = jnp.mean(vals_f32, axis=-1, keepdims=True)
    centered = vals_f32 - row_mean
    row_var = jnp.mean(centered * centered, axis=-1, keepdims=True)
    normed = centered * lax.rsqrt(row_var + EPS)
    return (normed * ln_scale + ln_bias).astype(BF16)


def row_of(ref):
    return ref[...].astype(F32)[None, :]


def attention_kernel(n_qkv, group, seq_ref, hid_ref, cos_ref, sin_ref, lns_ref, lnb_ref, bqkv_ref, wqkv_hbm, k_hbm, v_hbm, wout_hbm,
                     part_ref, kout_hbm, vout_hbm,
                     wqkv, kbuf, vbuf, wout, q_s, c_s, new_s, ctx, sem_w, sem_k, sem_v, sem_o, sem_ko, sem_vo):
    n_batch, s_max, head = kbuf.shape
    n_q = q_s.shape[1]
    d_model = wqkv.shape[0]
    n_groups = n_batch // group
    step = d_model // n_qkv
    for i in range(n_qkv):
        rows = pl.ds(i * step, step)
        pltpu.make_async_copy(wqkv_hbm.at[rows], wqkv.at[rows], sem_w.at[i]).start()
    for g in range(n_groups):
        rows = pl.ds(g * group, group)
        pltpu.make_async_copy(k_hbm.at[rows], kbuf.at[rows], sem_k.at[g]).start()
        pltpu.make_async_copy(v_hbm.at[rows], vbuf.at[rows], sem_v.at[g]).start()
    pltpu.make_async_copy(wout_hbm, wout, sem_o.at[0]).start()

    normed = row_norm(hid_ref[...].astype(F32), row_of(lns_ref), row_of(lnb_ref))
    acc = jnp.broadcast_to(row_of(bqkv_ref), (n_batch, wqkv.shape[1]))
    total = None
    for i in range(n_qkv):
        rows = pl.ds(i * step, step)
        pltpu.make_async_copy(wqkv_hbm.at[rows], wqkv.at[rows], sem_w.at[i]).wait()
        one = jnp.dot(normed[:, i * step:(i + 1) * step], wqkv[rows, :], preferred_element_type=F32)
        total = one if total is None else total + one
    qkv = (total + acc).astype(BF16).astype(F32)
    cos = jnp.concatenate([cos_ref[...], cos_ref[...]], axis=-1)
    sin = jnp.concatenate([-sin_ref[...], sin_ref[...]], axis=-1)
    for j in range(n_q + 1):
        x = qkv[:, j * head:(j + 1) * head]
        rot = x * cos + pltpu.roll(x, head // 2, 1) * sin
        if j < n_q:
            q_s[:, j, :] = rot
        else:
            new_s[0] = rot
    new_s[1] = qkv[:, (n_q + 1) * head:]

    row_iota = lax.broadcasted_iota(jnp.int32, (16, head), 0)
    lane_iota = lax.broadcasted_iota(jnp.int32, (n_q, s_max), 1)

    def one_group(g, carry):
        rows = pl.ds(g * group, group)
        pltpu.make_async_copy(k_hbm.at[rows], kbuf.at[rows], sem_k.at[g]).wait()
        pltpu.make_async_copy(v_hbm.at[rows], vbuf.at[rows], sem_v.at[g]).wait()
        scores = []
        for i in range(group):
            b = g * group + i
            p = seq_ref[b]
            base = pl.multiple_of((p // 16) * 16, 16)
            hit = row_iota == (p - base)
            for buf, which in ((kbuf, 0), (vbuf, 1)):
                old = buf[b, pl.ds(base, 16), :].astype(F32)
                row = new_s[which, pl.ds(b, 1), :]
                buf[b, pl.ds(base, 16), :] = jnp.where(hit, row, old).astype(BF16)
        pltpu.make_async_copy(kbuf.at[rows], kout_hbm.at[rows], sem_ko.at[g]).start()
        pltpu.make_async_copy(vbuf.at[rows], vout_hbm.at[rows], sem_vo.at[g]).start()
        for i in range(group):
            b = g * group + i
            s = lax.dot_general(q_s[b].astype(BF16), kbuf[b], NT, preferred_element_type=F32) * head ** -0.5
            scores.append(jnp.where(lane_iota <= seq_ref[b], s, -jnp.inf))
        s = jnp.concatenate(scores, axis=0)
        e = jnp.exp(s - jnp.max(s, axis=-1, keepdims=True))
        probs = (e / jnp.sum(e, axis=-1, keepdims=True))
        for i in range(group):
            b = g * group + i
            c_s[b] = jnp.dot(probs[i * n_q:(i + 1) * n_q].astype(BF16), vbuf[b], preferred_element_type=F32)
        return carry

    lax.fori_loop(0, n_groups, one_group, 0)
    for j in range(n_q):
        ctx[:, j * head:(j + 1) * head] = c_s[:, j, :].astype(BF16)
    pltpu.make_async_copy(wout_hbm, wout, sem_o.at[0]).wait()
    part = jnp.dot(ctx[...], wout[...], preferred_element_type=F32)
    part_ref[...] = part.reshape(part_ref.shape).astype(BF16)
    for g in range(n_groups):
        rows = pl.ds(g * group, group)
        pltpu.make_async_copy(kbuf.at[rows], kout_hbm.at[rows], sem_ko.at[g]).wait()
        pltpu.make_async_copy(vbuf.at[rows], vout_hbm.at[rows], sem_vo.at[g]).wait()


def moe_kernel(n_tp, n_x, n_cols, part_hbm, hid_hbm, ids_hbm, bout_hbm, lns_hbm, lnb_hbm, wr_hbm, wg_hbm, wu_hbm, wd_hbm,
               out_hbm,
               part, hid, ids, bout, lns, lnb, wr, wg, wu, wd, mask_s, a_recv, x1_s, ga, gb, h_t, g_t, act,
               o32, c0_send, c0_recv, c1_send, c1_own, c1_recv, c2_send, c2_own, c2_recv, outbuf,
               sem_in, sem_w, a_ss, a_rs, b1_ss, b1_rs, b2_ss, b2_rs, b3_ss, b3_rs,
               c0_ss, c0_rs, c1_ss, c1_rs, c2_ss, c2_rs, d_ss, d_rs, sem_out):
    t = lax.axis_index('tp')
    e = lax.axis_index('ep')
    x = e // 2
    c = e % 2
    n_exp, ff, d_model = wg.shape
    half = d_model // 2
    d_col = d_model // n_cols

    def y_peer(dt):
        return {'tp': lax.rem(t + dt, n_tp)}

    def y_src(dt):
        return lax.rem(t + n_tp - dt, n_tp)

    def x_dst(dx):
        return lax.rem(x + dx, n_x)

    def x_peer(dx):
        return {'ep': 2 * x_dst(dx) + c}

    def x_src(dx):
        return lax.rem(x + n_x - dx, n_x)

    partner = {'ep': 2 * x + 1 - c}

    def rcopy(src, dst, ss, rs, dev):
        return pltpu.make_async_remote_copy(src_ref=src, dst_ref=dst, send_sem=ss, recv_sem=rs, device_id=dev, device_id_type=MESH)

    small = [(part_hbm, part), (hid_hbm, hid), (ids_hbm, ids), (bout_hbm, bout), (lns_hbm, lns), (lnb_hbm, lnb), (wr_hbm, wr)]
    copies = [pltpu.make_async_copy(s, d, sem_in.at[i]) for i, (s, d) in enumerate(small)]
    for cp in copies:
        cp.start()
    n_pair = n_exp // 2

    def wcopy(w, p):
        src, dst = ((wg_hbm, wg), (wu_hbm, wu), (wd_hbm, wd))[w]
        rows = pl.ds(2 * p, 2)
        return pltpu.make_async_copy(src.at[rows], dst.at[rows], sem_w.at[w, p])

    for p in range(n_pair):
        wcopy(0, p).start()
        wcopy(1, p).start()
    for p in range(n_pair):
        wcopy(2, p).start()

    barrier = pltpu.get_barrier_semaphore()
    for dt in range(1, n_tp):
        pl.semaphore_signal(barrier, inc=1, device_id=y_peer(dt), device_id_type=MESH)
    for dx in range(1, n_x):
        pl.semaphore_signal(barrier, inc=1, device_id=x_peer(dx), device_id_type=MESH)
    pl.semaphore_signal(barrier, inc=1, device_id=partner, device_id_type=MESH)
    for cp in copies:
        cp.wait()
    pl.semaphore_wait(barrier, n_tp + n_x - 1)

    a_send = []
    for dt in range(1, n_tp):
        cp = rcopy(part.at[lax.rem(t + dt, n_tp)], a_recv.at[dt - 1], a_ss.at[dt - 1], a_rs.at[dt - 1], y_peer(dt))
        cp.start()
        a_send.append(cp)

    n_all = wr.shape[1]
    exp_iota = lax.broadcasted_iota(jnp.int32, (n_all, ids.shape[1]), 0)
    picked = jnp.zeros((n_all, ids.shape[1]), F32)
    for k in range(ids.shape[0]):
        picked = picked + jnp.where(exp_iota == ids[k:k + 1, :], 1.0, 0.0)
    mask_s[...] = picked.T.reshape(mask_s.shape)
    base = part[t].astype(F32)
    for dt in range(1, n_tp):
        a_send[dt - 1].wait_recv()
    for dt in range(1, n_tp):
        base = base + a_recv[dt - 1].astype(F32)
    x1 = (hid[t].astype(F32) + base + row_of(bout)).astype(BF16)
    x1_s[...] = x1
    h2 = row_norm(x1.astype(F32), row_of(lns), row_of(lnb))

    ga[x, c, t] = h2[:, :half]
    b_send = []

    def send(src, dst, ss, rs, dev):
        cp = rcopy(src, dst, ss, rs, dev)
        cp.start()
        b_send.append(cp)
        return cp

    a1 = [send(ga.at[x, c, t], ga.at[x, c, t], b1_ss.at[0, dt - 1], b1_rs.at[0, dt - 1], y_peer(dt)) for dt in range(1, n_tp)]
    logits = jnp.dot(h2, wr[...], preferred_element_type=F32)
    keep = mask_s[t] > 0.5
    logits = jnp.where(keep, logits, -jnp.inf)
    ex = jnp.exp(logits - jnp.max(logits, axis=-1, keepdims=True))
    gates = (ex / jnp.sum(ex, axis=-1, keepdims=True)).astype(BF16)
    gb[x, c, t, :, 0:half] = h2[:, half:]
    gb[x, c, t, :, half:half + n_all] = gates
    b1 = [send(gb.at[x, c, t], gb.at[x, c, t], b1_ss.at[1, dx - 1], b1_rs.at[1, dx - 1], x_peer(dx)) for dx in range(1, n_x)]
    for cp in a1:
        cp.wait_recv()
    a2 = [send(ga.at[x, c], ga.at[x, c], b2_ss.at[0, dx - 1], b2_rs.at[0, dx - 1], x_peer(dx)) for dx in range(1, n_x)]
    a3 = [send(ga.at[x, c], ga.at[x, c], b3_ss.at[0, 0], b3_rs.at[0, 0], partner)]
    for cp in b1:
        cp.wait_recv()
    b2 = [send(gb.at[:, c, t], gb.at[:, c, t], b2_ss.at[1, dt - 1], b2_rs.at[1, dt - 1], y_peer(dt)) for dt in range(1, n_tp)]
    b3 = [send(gb.at[:, c, t], gb.at[:, c, t], b3_ss.at[1, 0], b3_rs.at[1, 0], partner)]
    for dx in range(1, n_x):
        a2[dx - 1].wait_recv()
        xs = x_src(dx)
        a3.append(send(ga.at[xs, c], ga.at[xs, c], b3_ss.at[0, dx], b3_rs.at[0, dx], partner))
    for dt in range(1, n_tp):
        b2[dt - 1].wait_recv()
        ts = y_src(dt)
        b3.append(send(gb.at[:, c, ts], gb.at[:, c, ts], b3_ss.at[1, dt], b3_rs.at[1, dt], partner))
    for cp in a3:
        cp.wait_recv()
    n_tok = n_x * 2 * n_tp * x1.shape[0]
    for k in range(half // 256):
        piece = ga[:, :, :, :, k * 256:(k + 1) * 256].astype(F32).reshape(n_tok, 256)
        h_t[pl.ds(k * 256, 256), :] = piece.T.astype(BF16)
    for cp in b3:
        cp.wait_recv()
    for k in range(half // 256):
        piece = gb[:, :, :, :, k * 256:(k + 1) * 256].astype(F32).reshape(n_tok, 256)
        h_t[pl.ds(half + k * 256, 256), :] = piece.T.astype(BF16)
    g_t[...] = gb[:, :, :, :, half:half + n_all].astype(F32).reshape(n_tok, n_all).T

    def one_pair(p, carry):
        wcopy(0, p).wait()
        wcopy(1, p).wait()
        rows = pl.ds(2 * p, 2)
        gate_pre = jnp.dot(wg[rows].reshape(2 * ff, d_model), h_t[...], preferred_element_type=F32)
        up_pre = jnp.dot(wu[rows].reshape(2 * ff, d_model), h_t[...], preferred_element_type=F32)
        a = (gate_pre * jax.nn.sigmoid(gate_pre) * up_pre).astype(BF16).astype(F32)
        g0 = g_t[pl.ds(e * n_exp + 2 * p, 1), :]
        g1 = g_t[pl.ds(e * n_exp + 2 * p + 1, 1), :]
        a = jnp.concatenate([a[:ff] * g0, a[ff:] * g1], axis=0)
        act[p] = a.T.astype(BF16)
        return carry

    lax.fori_loop(0, n_pair, one_pair, 0)
    for p in range(n_pair):
        wcopy(2, p).wait()

    c_send = []

    def csend(src, dst, ss, rs, dev):
        cp = rcopy(src, dst, ss, rs, dev)
        cp.start()
        c_send.append(cp)
        return cp

    c0, c1, c2, dd = {}, {}, {}, {}

    def down(j):
        cols = slice(j * d_col, (j + 1) * d_col)
        o = None
        for p in range(n_pair):
            one = jnp.dot(act[p], wd[2 * p:2 * p + 2, :, cols].reshape(2 * ff, d_col), preferred_element_type=F32)
            o = one if o is None else o + one
        o = o.reshape(n_x, 2, n_tp, n_tok // (2 * n_x * n_tp), d_col)
        o32[j] = o
        c0_send[j] = o.astype(BF16)
        c0[j] = csend(c0_send.at[j, :, 1 - c], c0_recv.at[j], c0_ss.at[j], c0_rs.at[j], partner)

    def stage1(j):
        c0[j].wait_recv()
        s = o32[j, :, c] + c0_recv[j].astype(F32)
        c1_send[j] = s.astype(BF16)
        c1_own[j] = s
        if j < n_cols // 2:
            c1[j] = [csend(c1_send.at[j, x_dst(dx)], c1_recv.at[j, dx - 1], c1_ss.at[j, dx - 1], c1_rs.at[j, dx - 1], x_peer(dx)) for dx in range(1, n_x)]
        else:
            c1[j] = [csend(c1_send.at[j, :, lax.rem(t + dt, n_tp)], c1_recv.at[j, dt - 1], c1_ss.at[j, dt - 1], c1_rs.at[j, dt - 1], y_peer(dt)) for dt in range(1, n_tp)]

    def stage2(j):
        for cp in c1[j]:
            cp.wait_recv()
        s = c1_own[j, x] if j < n_cols // 2 else c1_own[j, :, t]
        for i in range(len(c1[j])):
            s = s + c1_recv[j, i].astype(F32)
        c2_send[j] = s.astype(BF16)
        c2_own[j] = s
        if j < n_cols // 2:
            c2[j] = [csend(c2_send.at[j, lax.rem(t + dt, n_tp)], c2_recv.at[j, dt - 1], c2_ss.at[j, dt - 1], c2_rs.at[j, dt - 1], y_peer(dt)) for dt in range(1, n_tp)]
        else:
            c2[j] = [csend(c2_send.at[j, x_dst(dx)], c2_recv.at[j, dx - 1], c2_ss.at[j, dx - 1], c2_rs.at[j, dx - 1], x_peer(dx)) for dx in range(1, n_x)]

    def stage3(j):
        for cp in c2[j]:
            cp.wait_recv()
        s = c2_own[j, t] if j < n_cols // 2 else c2_own[j, x]
        for i in range(len(c2[j])):
            s = s + c2_recv[j, i].astype(F32)
        cols = slice(j * d_col, (j + 1) * d_col)
        outbuf[j, t] = (x1_s[:, cols].astype(F32) + s).astype(BF16)
        dd[j] = [csend(outbuf.at[j, t], outbuf.at[j, t], d_ss.at[j, dt - 1], d_rs.at[j, dt - 1], y_peer(dt)) for dt in range(1, n_tp)]

    for j in range(n_cols + 3):
        if j < n_cols:
            down(j)
        if 0 <= j - 1 < n_cols:
            stage1(j - 1)
        if 0 <= j - 2 < n_cols:
            stage2(j - 2)
        if 0 <= j - 3 < n_cols:
            stage3(j - 3)
    outs = []
    for j in range(n_cols):
        for cp in dd[j]:
            cp.wait_recv()
        cp = pltpu.make_async_copy(outbuf.at[j], out_hbm.at[:, :, pl.ds(j * d_col, d_col)], sem_out.at[j])
        cp.start()
        outs.append(cp)
    for cp in a_send + b_send + c_send:
        cp.wait_send()
    for cp in outs:
        cp.wait()


def solution(mesh):
    n_ep = mesh.shape['ep']
    n_tp = mesh.shape['tp']
    n_x = n_ep // 2
    token_rows = P(('dp', 'ep'), None)
    token_vec = P(('dp', 'ep'))
    cache_spec = P(('dp', 'ep'), None, 'tp', None)
    expert_in = P('ep', None, 'tp')
    expert_down = P('ep', 'tp', None)
    any_spec = pl.BlockSpec(memory_space=pl.ANY)
    vmem = pl.BlockSpec(memory_space=pltpu.VMEM)
    smem = pl.BlockSpec(memory_space=pltpu.SMEM)

    def device_step(hidden, seq_lens, rope_cos, rope_sin, ln1_scale, ln1_bias, w_qkv, b_qkv, w_out, b_out, k_cache, v_cache, ln2_scale, ln2_bias, w_router, expert_ids, w_gate, w_up, w_down):
        n_batch, d_model = hidden.shape
        _, s_max, n_kv, head = k_cache.shape
        n_q = w_qkv.shape[1] // head - 2
        rows = n_batch // n_tp
        n_qkv, group = 4, 8
        k3 = k_cache.reshape(n_batch, s_max, head)
        v3 = v_cache.reshape(n_batch, s_max, head)
        dma = pltpu.SemaphoreType.DMA
        part, k_out, v_out = pl.pallas_call(
            functools.partial(attention_kernel, n_qkv, group),
            out_shape=(jax.ShapeDtypeStruct((n_tp, rows, d_model), BF16), jax.ShapeDtypeStruct(k3.shape, BF16), jax.ShapeDtypeStruct(v3.shape, BF16)),
            in_specs=[smem] + [vmem] * 6 + [any_spec] * 4,
            out_specs=(vmem, any_spec, any_spec),
            scratch_shapes=[
                pltpu.VMEM(w_qkv.shape, BF16),
                pltpu.VMEM(k3.shape, BF16),
                pltpu.VMEM(v3.shape, BF16),
                pltpu.VMEM(w_out.shape, BF16),
                pltpu.VMEM((n_batch, n_q, head), F32),
                pltpu.VMEM((n_batch, n_q, head), F32),
                pltpu.VMEM((2, n_batch, head), F32),
                pltpu.VMEM((n_batch, n_q * head), BF16),
                dma((n_qkv,)), dma((n_batch // group,)), dma((n_batch // group,)), dma((1,)), dma((n_batch // group,)), dma((n_batch // group,)),
            ],
            compiler_params=pltpu.CompilerParams(vmem_limit_bytes=40 * 1024 * 1024),
            name='attention',
        )(seq_lens, hidden, rope_cos, rope_sin, ln1_scale, ln1_bias, b_qkv, w_qkv, k3, v3, w_out)

        n_cols = 4
        d_col = d_model // n_cols
        half = d_model // 2
        wg = jnp.swapaxes(w_gate, 1, 2)
        wu = jnp.swapaxes(w_up, 1, 2)
        n_exp, ff, _ = wg.shape
        n_all = w_router.shape[1]
        n_tok = n_ep * n_batch
        n_pair = n_exp // 2
        ids_t = expert_ids.T
        V = pltpu.VMEM
        m = max(n_tp, n_x)
        assert n_tp == n_x
        out = pl.pallas_call(
            functools.partial(moe_kernel, n_tp, n_x, n_cols),
            out_shape=jax.ShapeDtypeStruct((n_tp, rows, d_model), BF16),
            in_specs=[any_spec] * 10,
            out_specs=any_spec,
            scratch_shapes=[
                V((n_tp, rows, d_model), BF16), V((n_tp, rows, d_model), BF16), V(ids_t.shape, jnp.int32),
                V((d_model,), BF16), V((d_model,), BF16), V((d_model,), BF16), V(w_router.shape, BF16),
                V(wg.shape, BF16), V(wg.shape, BF16), V(wg.shape, BF16),
                V((n_tp, rows, n_all), F32),
                V((n_tp - 1, rows, d_model), BF16),
                V((rows, d_model), BF16),
                V((n_x, 2, n_tp, rows, half), BF16),
                V((n_x, 2, n_tp, rows, half + n_all), BF16),
                V((d_model, n_tok), BF16),
                V((n_all, n_tok), F32),
                V((n_pair, n_tok, 2 * ff), BF16),
                V((n_cols, n_x, 2, n_tp, rows, d_col), F32),
                V((n_cols, n_x, 2, n_tp, rows, d_col), BF16),
                V((n_cols, n_x, n_tp, rows, d_col), BF16),
                V((n_cols, n_x, n_tp, rows, d_col), BF16),
                V((n_cols, n_x, n_tp, rows, d_col), F32),
                V((n_cols, m - 1, m, rows, d_col), BF16),
                V((n_cols, m, rows, d_col), BF16),
                V((n_cols, m, rows, d_col), F32),
                V((n_cols, m - 1, rows, d_col), BF16),
                V((n_cols, n_tp, rows, d_col), BF16),
                dma((7,)), dma((3, n_pair)),
                dma((m - 1,)), dma((m - 1,)),
                dma((2, m - 1)), dma((2, m - 1)), dma((2, m - 1)), dma((2, m - 1)), dma((2, m)), dma((2, m)),
                dma((n_cols,)), dma((n_cols,)),
                dma((n_cols, m - 1)), dma((n_cols, m - 1)), dma((n_cols, m - 1)), dma((n_cols, m - 1)), dma((n_cols, m - 1)), dma((n_cols, m - 1)),
                dma((n_cols,)),
            ],
            compiler_params=pltpu.CompilerParams(vmem_limit_bytes=62 * 1024 * 1024, collective_id=0, has_side_effects=True),
            name='moe',
        )(part, hidden.reshape(n_tp, rows, d_model), ids_t, b_out, ln2_scale, ln2_bias, w_router, wg, wu, w_down)
        return out.reshape(n_batch, d_model), k_out.reshape(k_cache.shape), v_out.reshape(v_cache.shape)

    in_specs = (token_rows, token_vec, token_rows, token_rows, P(), P(), P(None, 'tp'), P('tp'), P('tp', None), P(), cache_spec, cache_spec, P(), P(), P(), token_rows, expert_in, expert_in, expert_down)
    return jax.shard_map(device_step, mesh=mesh, in_specs=in_specs, out_specs=(token_rows, cache_spec, cache_spec), check_vma=False)
```

```python
import functools

import jax
import jax.numpy as jnp
from jax import lax
from jax.experimental import pallas as pl
from jax.experimental.pallas import tpu as pltpu
from jax.sharding import PartitionSpec as P

EPS = 1e-5
F32 = jnp.float32
BF16 = jnp.bfloat16
MESH = pl.DeviceIdType.MESH
NT = (((1,), (1,)), ((), ()))


def row_norm(vals_f32, ln_scale, ln_bias):
    row_mean = jnp.mean(vals_f32, axis=-1, keepdims=True)
    centered = vals_f32 - row_mean
    row_var = jnp.mean(centered * centered, axis=-1, keepdims=True)
    normed = centered * lax.rsqrt(row_var + EPS)
    return (normed * ln_scale + ln_bias).astype(BF16)


def row_of(ref):
    return ref[...].astype(F32)[None, :]


def attention_kernel(n_qkv, group, seq_hbm, hid_hbm, cos_hbm, sin_hbm, lns_hbm, lnb_hbm, bqkv_hbm, wqkv_hbm, k_hbm, v_hbm, wout_hbm,
                     part_hbm, kout_hbm, vout_hbm,
                     seq_ref, hid_ref, cos_ref, sin_ref, lns_ref, lnb_ref, bqkv_ref, part_ref, sem_s, wqkv, kbuf, vbuf, wout, q_s, c_s, new_s, ctx, sem_w, sem_k, sem_v, sem_o, sem_ko, sem_vo):
    n_batch, s_max, head = kbuf.shape
    n_q = q_s.shape[1]
    d_model = wqkv.shape[0]
    n_groups = n_batch // group
    step = d_model // n_qkv
    small = [(hid_hbm, hid_ref), (lns_hbm, lns_ref), (lnb_hbm, lnb_ref), (bqkv_hbm, bqkv_ref), (cos_hbm, cos_ref), (sin_hbm, sin_ref), (seq_hbm, seq_ref)]
    small = [pltpu.make_async_copy(src, dst, sem_s.at[i]) for i, (src, dst) in enumerate(small)]
    for cp in small:
        cp.start()
    for i in range(n_qkv):
        rows = pl.ds(i * step, step)
        pltpu.make_async_copy(wqkv_hbm.at[rows], wqkv.at[rows], sem_w.at[i]).start()
    for g in range(n_groups):
        rows = pl.ds(g * group, group)
        pltpu.make_async_copy(k_hbm.at[rows], kbuf.at[rows], sem_k.at[g]).start()
        pltpu.make_async_copy(v_hbm.at[rows], vbuf.at[rows], sem_v.at[g]).start()
    pltpu.make_async_copy(wout_hbm, wout, sem_o.at[0]).start()

    for cp in small:
        cp.wait()
    normed = row_norm(hid_ref[...].astype(F32), row_of(lns_ref), row_of(lnb_ref))
    acc = jnp.broadcast_to(row_of(bqkv_ref), (n_batch, wqkv.shape[1]))
    total = None
    for i in range(n_qkv):
        rows = pl.ds(i * step, step)
        pltpu.make_async_copy(wqkv_hbm.at[rows], wqkv.at[rows], sem_w.at[i]).wait()
        one = jnp.dot(normed[:, i * step:(i + 1) * step], wqkv[rows, :], preferred_element_type=F32)
        total = one if total is None else total + one
    qkv = (total + acc).astype(BF16).astype(F32)
    cos = jnp.concatenate([cos_ref[...], cos_ref[...]], axis=-1)
    sin = jnp.concatenate([-sin_ref[...], sin_ref[...]], axis=-1)
    for j in range(n_q + 1):
        x = qkv[:, j * head:(j + 1) * head]
        rot = x * cos + pltpu.roll(x, head // 2, 1) * sin
        if j < n_q:
            q_s[:, j, :] = rot
        else:
            new_s[0] = rot
    new_s[1] = qkv[:, (n_q + 1) * head:]

    row_iota = lax.broadcasted_iota(jnp.int32, (16, head), 0)
    lane_iota = lax.broadcasted_iota(jnp.int32, (n_q, s_max), 1)

    def one_group(g, carry):
        rows = pl.ds(g * group, group)
        pltpu.make_async_copy(k_hbm.at[rows], kbuf.at[rows], sem_k.at[g]).wait()
        pltpu.make_async_copy(v_hbm.at[rows], vbuf.at[rows], sem_v.at[g]).wait()
        scores = []
        for i in range(group):
            b = g * group + i
            p = seq_ref[b]
            base = pl.multiple_of((p // 16) * 16, 16)
            hit = row_iota == (p - base)
            for buf, which in ((kbuf, 0), (vbuf, 1)):
                old = buf[b, pl.ds(base, 16), :].astype(F32)
                row = new_s[which, pl.ds(b, 1), :]
                buf[b, pl.ds(base, 16), :] = jnp.where(hit, row, old).astype(BF16)
        pltpu.make_async_copy(kbuf.at[rows], kout_hbm.at[rows], sem_ko.at[g]).start()
        pltpu.make_async_copy(vbuf.at[rows], vout_hbm.at[rows], sem_vo.at[g]).start()
        for i in range(group):
            b = g * group + i
            s = lax.dot_general(q_s[b].astype(BF16), kbuf[b], NT, preferred_element_type=F32) * head ** -0.5
            scores.append(jnp.where(lane_iota <= seq_ref[b], s, -jnp.inf))
        s = jnp.concatenate(scores, axis=0)
        e = jnp.exp(s - jnp.max(s, axis=-1, keepdims=True))
        probs = (e / jnp.sum(e, axis=-1, keepdims=True))
        for i in range(group):
            b = g * group + i
            c_s[b] = jnp.dot(probs[i * n_q:(i + 1) * n_q].astype(BF16), vbuf[b], preferred_element_type=F32)
        return carry

    lax.fori_loop(0, n_groups, one_group, 0)
    for j in range(n_q):
        ctx[:, j * head:(j + 1) * head] = c_s[:, j, :].astype(BF16)
    pltpu.make_async_copy(wout_hbm, wout, sem_o.at[0]).wait()
    part = jnp.dot(ctx[...], wout[...], preferred_element_type=F32)
    part_ref[...] = part.reshape(part_ref.shape).astype(BF16)
    out_copy = pltpu.make_async_copy(part_ref, part_hbm, sem_s.at[0])
    out_copy.start()
    for g in range(n_groups):
        rows = pl.ds(g * group, group)
        pltpu.make_async_copy(kbuf.at[rows], kout_hbm.at[rows], sem_ko.at[g]).wait()
        pltpu.make_async_copy(vbuf.at[rows], vout_hbm.at[rows], sem_vo.at[g]).wait()
    out_copy.wait()


def moe_kernel(n_tp, n_x, n_cols, part_hbm, hid_hbm, ids_hbm, bout_hbm, lns_hbm, lnb_hbm, wr_hbm, wg_hbm, wu_hbm, wd_hbm,
               out_hbm,
               part, hid, ids, bout, lns, lnb, wr, wg, wu, wd, mask_s, a_recv, x1_s, ga, gb, h_t, g_t, act,
               o32, c0_send, c0_recv, c1_send, c1_own, c1_recv, c2_send, c2_own, c2_recv, outbuf,
               sem_in, sem_w, a_ss, a_rs, b1_ss, b1_rs, b2_ss, b2_rs, b3_ss, b3_rs,
               c0_ss, c0_rs, c1_ss, c1_rs, c2_ss, c2_rs, d_ss, d_rs, sem_out):
    t = lax.axis_index('tp')
    e = lax.axis_index('ep')
    x = e // 2
    c = e % 2
    n_exp, ff, d_model = wg.shape
    half = d_model // 2
    d_col = d_model // n_cols

    def y_peer(dt):
        return {'tp': lax.rem(t + dt, n_tp)}

    def y_src(dt):
        return lax.rem(t + n_tp - dt, n_tp)

    def x_dst(dx):
        return lax.rem(x + dx, n_x)

    def x_peer(dx):
        return {'ep': 2 * x_dst(dx) + c}

    def x_src(dx):
        return lax.rem(x + n_x - dx, n_x)

    partner = {'ep': 2 * x + 1 - c}

    def rcopy(src, dst, ss, rs, dev):
        return pltpu.make_async_remote_copy(src_ref=src, dst_ref=dst, send_sem=ss, recv_sem=rs, device_id=dev, device_id_type=MESH)

    small = [(part_hbm, part), (hid_hbm, hid), (ids_hbm, ids), (bout_hbm, bout), (lns_hbm, lns), (lnb_hbm, lnb), (wr_hbm, wr)]
    copies = [pltpu.make_async_copy(s, d, sem_in.at[i]) for i, (s, d) in enumerate(small)]
    for cp in copies:
        cp.start()
    n_pair = n_exp // 2

    def wcopy(w, p):
        src, dst = ((wg_hbm, wg), (wu_hbm, wu), (wd_hbm, wd))[w]
        rows = pl.ds(2 * p, 2)
        return pltpu.make_async_copy(src.at[rows], dst.at[rows], sem_w.at[w, p])

    barrier = pltpu.get_barrier_semaphore()
    for dt in range(1, n_tp):
        pl.semaphore_signal(barrier, inc=1, device_id=y_peer(dt), device_id_type=MESH)
    for dx in range(1, n_x):
        pl.semaphore_signal(barrier, inc=1, device_id=x_peer(dx), device_id_type=MESH)
    pl.semaphore_signal(barrier, inc=1, device_id=partner, device_id_type=MESH)
    for cp in copies:
        cp.wait()
    for p in range(n_pair):
        wcopy(0, p).start()
        wcopy(1, p).start()
    for p in range(n_pair):
        wcopy(2, p).start()
    pl.semaphore_wait(barrier, n_tp + n_x - 1)

    a_send = []
    for dt in range(1, n_tp):
        cp = rcopy(part.at[lax.rem(t + dt, n_tp)], a_recv.at[dt - 1], a_ss.at[dt - 1], a_rs.at[dt - 1], y_peer(dt))
        cp.start()
        a_send.append(cp)

    n_all = wr.shape[1]
    exp_iota = lax.broadcasted_iota(jnp.int32, (n_all, ids.shape[1]), 0)
    picked = jnp.zeros((n_all, ids.shape[1]), F32)
    for k in range(ids.shape[0]):
        picked = picked + jnp.where(exp_iota == ids[k:k + 1, :], 1.0, 0.0)
    mask_s[...] = picked.T.reshape(mask_s.shape)
    base = part[t].astype(F32)
    for dt in range(1, n_tp):
        a_send[dt - 1].wait_recv()
    for dt in range(1, n_tp):
        base = base + a_recv[dt - 1].astype(F32)
    x1 = (hid[t].astype(F32) + base + row_of(bout)).astype(BF16)
    x1_s[...] = x1
    h2 = row_norm(x1.astype(F32), row_of(lns), row_of(lnb))

    ga[x, c, t] = h2[:, :half]
    b_send = []

    def send(src, dst, ss, rs, dev):
        cp = rcopy(src, dst, ss, rs, dev)
        cp.start()
        b_send.append(cp)
        return cp

    a1 = [send(ga.at[x, c, t], ga.at[x, c, t], b1_ss.at[0, dt - 1], b1_rs.at[0, dt - 1], y_peer(dt)) for dt in range(1, n_tp)]
    logits = jnp.dot(h2, wr[...], preferred_element_type=F32)
    keep = mask_s[t] > 0.5
    logits = jnp.where(keep, logits, -jnp.inf)
    ex = jnp.exp(logits - jnp.max(logits, axis=-1, keepdims=True))
    gates = (ex / jnp.sum(ex, axis=-1, keepdims=True)).astype(BF16)
    gb[x, c, t, :, 0:half] = h2[:, half:]
    gb[x, c, t, :, half:half + n_all] = gates
    b1 = [send(gb.at[x, c, t], gb.at[x, c, t], b1_ss.at[1, dx - 1], b1_rs.at[1, dx - 1], x_peer(dx)) for dx in range(1, n_x)]
    for cp in a1:
        cp.wait_recv()
    a2 = [send(ga.at[x, c], ga.at[x, c], b2_ss.at[0, dx - 1], b2_rs.at[0, dx - 1], x_peer(dx)) for dx in range(1, n_x)]
    a3 = [send(ga.at[x, c], ga.at[x, c], b3_ss.at[0, 0], b3_rs.at[0, 0], partner)]
    for cp in b1:
        cp.wait_recv()
    b2 = [send(gb.at[:, c, t], gb.at[:, c, t], b2_ss.at[1, dt - 1], b2_rs.at[1, dt - 1], y_peer(dt)) for dt in range(1, n_tp)]
    b3 = [send(gb.at[:, c, t], gb.at[:, c, t], b3_ss.at[1, 0], b3_rs.at[1, 0], partner)]
    for dx in range(1, n_x):
        a2[dx - 1].wait_recv()
        xs = x_src(dx)
        a3.append(send(ga.at[xs, c], ga.at[xs, c], b3_ss.at[0, dx], b3_rs.at[0, dx], partner))
    for dt in range(1, n_tp):
        b2[dt - 1].wait_recv()
        ts = y_src(dt)
        b3.append(send(gb.at[:, c, ts], gb.at[:, c, ts], b3_ss.at[1, dt], b3_rs.at[1, dt], partner))
    for cp in a3:
        cp.wait_recv()
    n_tok = n_x * 2 * n_tp * x1.shape[0]
    for k in range(half // 256):
        piece = ga[:, :, :, :, k * 256:(k + 1) * 256].astype(F32).reshape(n_tok, 256)
        h_t[pl.ds(k * 256, 256), :] = piece.T.astype(BF16)
    for cp in b3:
        cp.wait_recv()
    for k in range(half // 256):
        piece = gb[:, :, :, :, k * 256:(k + 1) * 256].astype(F32).reshape(n_tok, 256)
        h_t[pl.ds(half + k * 256, 256), :] = piece.T.astype(BF16)
    g_t[...] = gb[:, :, :, :, half:half + n_all].astype(F32).reshape(n_tok, n_all).T

    def one_pair(p, carry):
        wcopy(0, p).wait()
        wcopy(1, p).wait()
        rows = pl.ds(2 * p, 2)
        gate_pre = jnp.dot(wg[rows].reshape(2 * ff, d_model), h_t[...], preferred_element_type=F32)
        up_pre = jnp.dot(wu[rows].reshape(2 * ff, d_model), h_t[...], preferred_element_type=F32)
        a = (gate_pre * jax.nn.sigmoid(gate_pre) * up_pre).astype(BF16).astype(F32)
        g0 = g_t[pl.ds(e * n_exp + 2 * p, 1), :]
        g1 = g_t[pl.ds(e * n_exp + 2 * p + 1, 1), :]
        a = jnp.concatenate([a[:ff] * g0, a[ff:] * g1], axis=0)
        act[:, pl.ds(pl.multiple_of(2 * ff * p, 2 * ff), 2 * ff)] = a.T.astype(BF16)
        return carry

    lax.fori_loop(0, n_pair, one_pair, 0, unroll=2)
    for p in range(n_pair):
        wcopy(2, p).wait()

    c_send = []

    def csend(src, dst, ss, rs, dev):
        cp = rcopy(src, dst, ss, rs, dev)
        cp.start()
        c_send.append(cp)
        return cp

    c0, c1, c2, dd = {}, {}, {}, {}
    d_half = d_col // 2

    def down(j):
        cols = slice(j * d_col, (j + 1) * d_col)
        o = jnp.dot(act[...], wd[:, :, cols].reshape(n_exp * ff, d_col), preferred_element_type=F32)
        for h in range(2):
            piece = o[:, h * d_half:(h + 1) * d_half].reshape(n_x, 2, n_tp, n_tok // (2 * n_x * n_tp), d_half)
            o32[j, h] = piece
            c0_send[j, h] = piece.astype(BF16)
        c0[j] = csend(c0_send.at[j, :, :, 1 - c], c0_recv.at[j], c0_ss.at[j], c0_rs.at[j], partner)

    def x_send(src, dst, ss, rs, j, h):
        return [csend(src(x_dst(dx)), dst.at[j, h, dx - 1], ss.at[j, h, dx - 1], rs.at[j, h, dx - 1], x_peer(dx)) for dx in range(1, n_x)]

    def y_send(src, dst, ss, rs, j, h):
        return [csend(src(lax.rem(t + dt, n_tp)), dst.at[j, h, dt - 1], ss.at[j, h, dt - 1], rs.at[j, h, dt - 1], y_peer(dt)) for dt in range(1, n_tp)]

    def stage1(j):
        c0[j].wait_recv()
        for h in range(2):
            s = o32[j, h, :, c] + c0_recv[j, h].astype(F32)
            c1_send[j, h] = s.astype(BF16)
            c1_own[j, h] = s
        c1[j, 0] = x_send(lambda i: c1_send.at[j, 0, i], c1_recv, c1_ss, c1_rs, j, 0)
        c1[j, 1] = y_send(lambda i: c1_send.at[j, 1, :, i], c1_recv, c1_ss, c1_rs, j, 1)

    def stage2(j):
        for h in range(2):
            for cp in c1[j, h]:
                cp.wait_recv()
            s = c1_own[j, 1, :, t] if h else c1_own[j, 0, x]
            for i in range(len(c1[j, h])):
                s = s + c1_recv[j, h, i].astype(F32)
            c2_send[j, h] = s.astype(BF16)
            c2_own[j, h] = s
            if h:
                c2[j, 1] = x_send(lambda i: c2_send.at[j, 1, i], c2_recv, c2_ss, c2_rs, j, 1)
            else:
                c2[j, 0] = y_send(lambda i: c2_send.at[j, 0, i], c2_recv, c2_ss, c2_rs, j, 0)

    def stage3(j):
        for h in range(2):
            for cp in c2[j, h]:
                cp.wait_recv()
            s = c2_own[j, 1, x] if h else c2_own[j, 0, t]
            for i in range(len(c2[j, h])):
                s = s + c2_recv[j, h, i].astype(F32)
            cols = slice(j * d_col + h * d_half, j * d_col + (h + 1) * d_half)
            outbuf[j, t, :, h * d_half:(h + 1) * d_half] = (x1_s[:, cols].astype(F32) + s).astype(BF16)
        dd[j] = [csend(outbuf.at[j, t], outbuf.at[j, t], d_ss.at[j, dt - 1], d_rs.at[j, dt - 1], y_peer(dt)) for dt in range(1, n_tp)]

    plan = [(stage, j, pos) for j in range(n_cols) for stage, pos in ((down, j), (stage1, j + 1.25 if j < n_cols - 1 else j + 0.5), (stage2, j + 3.5), (stage3, j + 5.75))]
    for stage, j, _ in sorted(plan, key=lambda one: one[2]):
        stage(j)
    outs = []
    for j in range(n_cols):
        for cp in dd[j]:
            cp.wait_recv()
        cp = pltpu.make_async_copy(outbuf.at[j], out_hbm.at[:, :, pl.ds(j * d_col, d_col)], sem_out.at[j])
        cp.start()
        outs.append(cp)
    for cp in a_send + b_send + c_send:
        cp.wait_send()
    for cp in outs:
        cp.wait()


def solution(mesh):
    n_ep = mesh.shape['ep']
    n_tp = mesh.shape['tp']
    n_x = n_ep // 2
    token_rows = P(('dp', 'ep'), None)
    token_vec = P(('dp', 'ep'))
    cache_spec = P(('dp', 'ep'), None, 'tp', None)
    expert_in = P('ep', None, 'tp')
    expert_down = P('ep', 'tp', None)
    hbm_spec = pl.BlockSpec(memory_space=pltpu.HBM)

    def device_step(hidden, seq_lens, rope_cos, rope_sin, ln1_scale, ln1_bias, w_qkv, b_qkv, w_out, b_out, k_cache, v_cache, ln2_scale, ln2_bias, w_router, expert_ids, w_gate, w_up, w_down):
        n_batch, d_model = hidden.shape
        _, s_max, n_kv, head = k_cache.shape
        n_q = w_qkv.shape[1] // head - 2
        rows = n_batch // n_tp
        n_qkv, group = 4, 8
        k3 = k_cache.reshape(n_batch, s_max, head)
        v3 = v_cache.reshape(n_batch, s_max, head)
        dma = pltpu.SemaphoreType.DMA
        part, k_out, v_out = pl.pallas_call(
            functools.partial(attention_kernel, n_qkv, group),
            out_shape=(jax.ShapeDtypeStruct((n_tp, rows, d_model), BF16), jax.ShapeDtypeStruct(k3.shape, BF16), jax.ShapeDtypeStruct(v3.shape, BF16)),
            in_specs=[hbm_spec] * 11,
            out_specs=(hbm_spec,) * 3,
            scratch_shapes=[
                pltpu.SMEM(seq_lens.shape, jnp.int32),
                pltpu.VMEM(hidden.shape, BF16),
                pltpu.VMEM(rope_cos.shape, F32),
                pltpu.VMEM(rope_sin.shape, F32),
                pltpu.VMEM((d_model,), BF16),
                pltpu.VMEM((d_model,), BF16),
                pltpu.VMEM(b_qkv.shape, BF16),
                pltpu.VMEM((n_tp, rows, d_model), BF16),
                dma((7,)),
                pltpu.VMEM(w_qkv.shape, BF16),
                pltpu.VMEM(k3.shape, BF16),
                pltpu.VMEM(v3.shape, BF16),
                pltpu.VMEM(w_out.shape, BF16),
                pltpu.VMEM((n_batch, n_q, head), F32),
                pltpu.VMEM((n_batch, n_q, head), F32),
                pltpu.VMEM((2, n_batch, head), F32),
                pltpu.VMEM((n_batch, n_q * head), BF16),
                dma((n_qkv,)), dma((n_batch // group,)), dma((n_batch // group,)), dma((1,)), dma((n_batch // group,)), dma((n_batch // group,)),
            ],
            compiler_params=pltpu.CompilerParams(vmem_limit_bytes=63 * 1024 * 1024),
            name='attention',
        )(seq_lens, hidden, rope_cos, rope_sin, ln1_scale, ln1_bias, b_qkv, w_qkv, k3, v3, w_out)

        n_cols = 4
        d_col = d_model // n_cols
        d_half = d_col // 2
        half = d_model // 2
        wg = jnp.swapaxes(w_gate, 1, 2)
        wu = jnp.swapaxes(w_up, 1, 2)
        n_exp, ff, _ = wg.shape
        n_all = w_router.shape[1]
        n_tok = n_ep * n_batch
        n_pair = n_exp // 2
        ids_t = expert_ids.T
        V = pltpu.VMEM
        m = max(n_tp, n_x)
        assert n_tp == n_x
        out = pl.pallas_call(
            functools.partial(moe_kernel, n_tp, n_x, n_cols),
            out_shape=jax.ShapeDtypeStruct((n_tp, rows, d_model), BF16),
            in_specs=[hbm_spec] * 10,
            out_specs=hbm_spec,
            scratch_shapes=[
                V((n_tp, rows, d_model), BF16), V((n_tp, rows, d_model), BF16), V(ids_t.shape, jnp.int32),
                V((d_model,), BF16), V((d_model,), BF16), V((d_model,), BF16), V(w_router.shape, BF16),
                V(wg.shape, BF16), V(wg.shape, BF16), V(wg.shape, BF16),
                V((n_tp, rows, n_all), F32),
                V((n_tp - 1, rows, d_model), BF16),
                V((rows, d_model), BF16),
                V((n_x, 2, n_tp, rows, half), BF16),
                V((n_x, 2, n_tp, rows, half + n_all), BF16),
                V((d_model, n_tok), BF16),
                V((n_all, n_tok), F32),
                V((n_tok, n_exp * ff), BF16),
                V((n_cols, 2, n_x, 2, n_tp, rows, d_half), F32),
                V((n_cols, 2, n_x, 2, n_tp, rows, d_half), BF16),
                V((n_cols, 2, n_x, n_tp, rows, d_half), BF16),
                V((n_cols, 2, n_x, n_tp, rows, d_half), BF16),
                V((n_cols, 2, n_x, n_tp, rows, d_half), F32),
                V((n_cols, 2, m - 1, m, rows, d_half), BF16),
                V((n_cols, 2, m, rows, d_half), BF16),
                V((n_cols, 2, m, rows, d_half), F32),
                V((n_cols, 2, m - 1, rows, d_half), BF16),
                V((n_cols, n_tp, rows, d_col), BF16),
                dma((7,)), dma((3, n_pair)),
                dma((m - 1,)), dma((m - 1,)),
                dma((2, m - 1)), dma((2, m - 1)), dma((2, m - 1)), dma((2, m - 1)), dma((2, m)), dma((2, m)),
                dma((n_cols,)), dma((n_cols,)),
                dma((n_cols, 2, m - 1)), dma((n_cols, 2, m - 1)), dma((n_cols, 2, m - 1)), dma((n_cols, 2, m - 1)), dma((n_cols, m - 1)), dma((n_cols, m - 1)),
                dma((n_cols,)),
            ],
            compiler_params=pltpu.CompilerParams(vmem_limit_bytes=63 * 1024 * 1024, collective_id=0, has_side_effects=True),
            name='moe',
        )(part, hidden.reshape(n_tp, rows, d_model), ids_t, b_out, ln2_scale, ln2_bias, w_router, wg, wu, w_down)
        return out.reshape(n_batch, d_model), k_out.reshape(k_cache.shape), v_out.reshape(v_cache.shape)

    in_specs = (token_rows, token_vec, token_rows, token_rows, P(), P(), P(None, 'tp'), P('tp'), P('tp', None), P(), cache_spec, cache_spec, P(), P(), P(), token_rows, expert_in, expert_in, expert_down)
    return jax.shard_map(device_step, mesh=mesh, in_specs=in_specs, out_specs=(token_rows, cache_spec, cache_spec), check_vma=False)
```

```python
import functools

import jax
import jax.numpy as jnp
from jax import lax
from jax.experimental import pallas as pl
from jax.experimental.pallas import tpu as pltpu
from jax.sharding import PartitionSpec as P

EPS = 1e-5
F32 = jnp.float32
BF16 = jnp.bfloat16
MESH = pl.DeviceIdType.MESH
NT = (((1,), (1,)), ((), ()))


def row_norm(vals_f32, ln_scale, ln_bias):
    row_mean = jnp.mean(vals_f32, axis=-1, keepdims=True)
    centered = vals_f32 - row_mean
    row_var = jnp.mean(centered * centered, axis=-1, keepdims=True)
    normed = centered * lax.rsqrt(row_var + EPS)
    return (normed * ln_scale + ln_bias).astype(BF16)


def row_of(ref):
    return ref[...].astype(F32)[None, :]


def attention_kernel(n_qkv, group, seq_hbm, hid_hbm, cos_hbm, sin_hbm, lns_hbm, lnb_hbm, bqkv_hbm, wqkv_hbm, k_hbm, v_hbm,
                     ctx_hbm, kout_hbm, vout_hbm,
                     seq_ref, hid_ref, cos_ref, sin_ref, lns_ref, lnb_ref, bqkv_ref, sem_s, wqkv, kbuf, vbuf, q_s, c_s, new_s, ctx, sem_w, sem_k, sem_v, sem_ko, sem_vo):
    n_batch, s_max, head = kbuf.shape
    n_q = q_s.shape[1]
    d_model = wqkv.shape[0]
    n_groups = n_batch // group
    step = d_model // n_qkv
    small = [(hid_hbm, hid_ref), (lns_hbm, lns_ref), (lnb_hbm, lnb_ref), (bqkv_hbm, bqkv_ref), (cos_hbm, cos_ref), (sin_hbm, sin_ref), (seq_hbm, seq_ref)]
    small = [pltpu.make_async_copy(src, dst, sem_s.at[i]) for i, (src, dst) in enumerate(small)]
    for cp in small:
        cp.start()
    for i in range(n_qkv):
        rows = pl.ds(i * step, step)
        pltpu.make_async_copy(wqkv_hbm.at[rows], wqkv.at[rows], sem_w.at[i]).start()

    for cp in small:
        cp.wait()
    for g in range(n_groups):
        rows = pl.ds(g * group, group)
        pltpu.make_async_copy(k_hbm.at[rows], kbuf.at[rows], sem_k.at[g]).start()
        pltpu.make_async_copy(v_hbm.at[rows], vbuf.at[rows], sem_v.at[g]).start()
    normed = row_norm(hid_ref[...].astype(F32), row_of(lns_ref), row_of(lnb_ref))
    acc = jnp.broadcast_to(row_of(bqkv_ref), (n_batch, wqkv.shape[1]))
    total = None
    for i in range(n_qkv):
        rows = pl.ds(i * step, step)
        pltpu.make_async_copy(wqkv_hbm.at[rows], wqkv.at[rows], sem_w.at[i]).wait()
        one = jnp.dot(normed[:, i * step:(i + 1) * step], wqkv[rows, :], preferred_element_type=F32)
        total = one if total is None else total + one
    qkv = (total + acc).astype(BF16).astype(F32)
    cos = jnp.concatenate([cos_ref[...], cos_ref[...]], axis=-1)
    sin = jnp.concatenate([-sin_ref[...], sin_ref[...]], axis=-1)
    for j in range(n_q + 1):
        x = qkv[:, j * head:(j + 1) * head]
        rot = x * cos + pltpu.roll(x, head // 2, 1) * sin
        if j < n_q:
            q_s[:, j, :] = rot
        else:
            new_s[0] = rot
    new_s[1] = qkv[:, (n_q + 1) * head:]

    row_iota = lax.broadcasted_iota(jnp.int32, (16, head), 0)
    lane_iota = lax.broadcasted_iota(jnp.int32, (n_q, s_max), 1)

    def one_group(g, carry):
        rows = pl.ds(g * group, group)
        pltpu.make_async_copy(k_hbm.at[rows], kbuf.at[rows], sem_k.at[g]).wait()
        pltpu.make_async_copy(v_hbm.at[rows], vbuf.at[rows], sem_v.at[g]).wait()
        scores = []
        for i in range(group):
            b = g * group + i
            p = seq_ref[b]
            base = pl.multiple_of((p // 16) * 16, 16)
            hit = row_iota == (p - base)
            for buf, which in ((kbuf, 0), (vbuf, 1)):
                old = buf[b, pl.ds(base, 16), :].astype(F32)
                row = new_s[which, pl.ds(b, 1), :]
                buf[b, pl.ds(base, 16), :] = jnp.where(hit, row, old).astype(BF16)
        pltpu.make_async_copy(kbuf.at[rows], kout_hbm.at[rows], sem_ko.at[g]).start()
        pltpu.make_async_copy(vbuf.at[rows], vout_hbm.at[rows], sem_vo.at[g]).start()
        for i in range(group):
            b = g * group + i
            s = lax.dot_general(q_s[b].astype(BF16), kbuf[b], NT, preferred_element_type=F32) * head ** -0.5
            scores.append(jnp.where(lane_iota <= seq_ref[b], s, -jnp.inf))
        s = jnp.concatenate(scores, axis=0)
        e = jnp.exp(s - jnp.max(s, axis=-1, keepdims=True))
        probs = (e / jnp.sum(e, axis=-1, keepdims=True))
        for i in range(group):
            b = g * group + i
            c_s[b] = jnp.dot(probs[i * n_q:(i + 1) * n_q].astype(BF16), vbuf[b], preferred_element_type=F32)
        return carry

    lax.fori_loop(0, n_groups, one_group, 0)
    for j in range(n_q):
        ctx[:, j * head:(j + 1) * head] = c_s[:, j, :].astype(BF16)
    out_copy = pltpu.make_async_copy(ctx, ctx_hbm, sem_s.at[0])
    out_copy.start()
    for g in range(n_groups):
        rows = pl.ds(g * group, group)
        pltpu.make_async_copy(kbuf.at[rows], kout_hbm.at[rows], sem_ko.at[g]).wait()
        pltpu.make_async_copy(vbuf.at[rows], vout_hbm.at[rows], sem_vo.at[g]).wait()
    out_copy.wait()


def moe_kernel(n_tp, n_x, widths, ctx_hbm, hid_hbm, ids_hbm, bout_hbm, lns_hbm, lnb_hbm, wout_hbm, wr_hbm, wg_hbm, wu_hbm, wd_hbm,
               out_hbm,
               ctx, hid, ids, bout, lns, lnb, wout, wr, wg, wu, wd, mask_s, part, a_recv, x1_s, ga, gb, h_s, acc, act, outbuf, cbufs,
               sem_in, sem_o, sem_w, a_ss, a_rs, b1_ss, b1_rs, b2_ss, b2_rs, b3_ss, b3_rs, x_ss, x_rs,
               c0_ss, c0_rs, c1_ss, c1_rs, c2_ss, c2_rs, sem_out):
    t = lax.axis_index('tp')
    e = lax.axis_index('ep')
    x = e // 2
    c = e % 2
    n_exp, ff, d_model = wg.shape
    n_all = wr.shape[1]
    rows = x1_s.shape[1]
    n_tok = h_s.shape[0]
    n_k, quarter = ga.shape[0], ga.shape[-1]
    k_cols = 2 * quarter
    n_cols = len(widths)
    starts = [sum(widths[:j]) for j in range(n_cols)]

    def y_dst(dt):
        return lax.rem(t + dt, n_tp)

    def y_peer(dt):
        return {'tp': y_dst(dt)}

    def y_src(dt):
        return lax.rem(t + n_tp - dt, n_tp)

    def x_dst(dx):
        return lax.rem(x + dx, n_x)

    def x_peer(dx):
        return {'ep': 2 * x_dst(dx) + c}

    def x_src(dx):
        return lax.rem(x + n_x - dx, n_x)

    partner = {'ep': 2 * x + 1 - c}
    sent = []

    def send(src, dst, ss, rs, dev):
        cp = pltpu.make_async_remote_copy(src_ref=src, dst_ref=dst, send_sem=ss, recv_sem=rs, device_id=dev, device_id_type=MESH)
        cp.start()
        sent.append(cp)
        return cp

    small = [(ctx_hbm, ctx), (ids_hbm, ids), (hid_hbm.at[t], hid), (bout_hbm, bout), (lns_hbm, lns), (lnb_hbm, lnb)]
    copies = [pltpu.make_async_copy(src, dst, sem_in.at[i]) for i, (src, dst) in enumerate(small)]
    for cp in copies:
        cp.start()
    n_o = part.shape[0]
    o_cols = d_model // n_o
    o_copies = [pltpu.make_async_copy(wout_hbm.at[:, pl.ds(i * o_cols, o_cols)], wout.at[:, pl.ds(i * o_cols, o_cols)], sem_o.at[i]) for i in range(n_o)]
    for cp in o_copies:
        cp.start()
    r_copy = pltpu.make_async_copy(wr_hbm, wr, sem_in.at[len(small)])
    r_copy.start()

    barrier = pltpu.get_barrier_semaphore()
    for dt in range(1, n_tp):
        pl.semaphore_signal(barrier, inc=1, device_id=y_peer(dt), device_id_type=MESH)
    for dx in range(1, n_x):
        pl.semaphore_signal(barrier, inc=1, device_id=x_peer(dx), device_id_type=MESH)
    pl.semaphore_signal(barrier, inc=1, device_id=partner, device_id_type=MESH)
    n_pair = n_exp // 2

    def wcopy(w, p):
        src, dst = ((wg_hbm, wg), (wu_hbm, wu), (wd_hbm, wd))[w]
        pair = pl.ds(2 * p, 2)
        return pltpu.make_async_copy(src.at[pair], dst.at[pair], sem_w.at[w, p])

    for cp in copies:
        cp.wait()
    exp_iota = lax.broadcasted_iota(jnp.int32, (n_all, ids.shape[1]), 0)
    picked = jnp.zeros((n_all, ids.shape[1]), F32)
    for k in range(ids.shape[0]):
        picked = picked + jnp.where(exp_iota == ids[k:k + 1, :], 1.0, 0.0)
    mask_s[...] = picked.T.reshape(mask_s.shape)
    pl.semaphore_wait(barrier, n_tp + n_x - 1)
    a = []
    for i in range(n_o):
        o_copies[i].wait()
        if i == n_o - 1:
            r_copy.wait()
            for p in range(n_pair):
                wcopy(0, p).start()
                wcopy(1, p).start()
            for p in range(n_pair):
                wcopy(2, p).start()
        o = jnp.dot(ctx[...], wout[:, i * o_cols:(i + 1) * o_cols], preferred_element_type=F32)
        part[i] = o.reshape(n_tp, rows, o_cols).astype(BF16)
        a.append([send(part.at[i, y_dst(dt)], a_recv.at[i, dt - 1], a_ss.at[i, dt - 1], a_rs.at[i, dt - 1], y_peer(dt)) for dt in range(1, n_tp)])
    sums = []
    for i in range(n_o):
        total = part[i, t].astype(F32)
        for dt in range(1, n_tp):
            a[i][dt - 1].wait_recv()
            total = total + a_recv[i, dt - 1].astype(F32)
        sums.append(total)
    x1 = (hid[...].astype(F32) + jnp.concatenate(sums, axis=-1) + row_of(bout)).astype(BF16)
    x1_s[t] = x1
    h2 = row_norm(x1.astype(F32), row_of(lns), row_of(lnb))
    b1, b2, b3 = {}, {}, {}

    def first(k):
        lo = k * k_cols
        ga[k, x, c, t] = h2[:, lo:lo + quarter]
        gb[k, x, c, t, :, 0:quarter] = h2[:, lo + quarter:lo + k_cols]
        b1[k, 0] = [send(ga.at[k, x, c, t], ga.at[k, x, c, t], b1_ss.at[k, 0, dt - 1], b1_rs.at[k, 0, dt - 1], y_peer(dt)) for dt in range(1, n_tp)]
        b1[k, 1] = [send(gb.at[k, x, c, t], gb.at[k, x, c, t], b1_ss.at[k, 1, dx - 1], b1_rs.at[k, 1, dx - 1], x_peer(dx)) for dx in range(1, n_x)]

    def second(k):
        for cp in b1[k, 0]:
            cp.wait_recv()
        b2[k, 0] = [send(ga.at[k, x, c], ga.at[k, x, c], b2_ss.at[k, 0, dx - 1], b2_rs.at[k, 0, dx - 1], x_peer(dx)) for dx in range(1, n_x)]
        for cp in b1[k, 1]:
            cp.wait_recv()
        b2[k, 1] = [send(gb.at[k, :, c, t], gb.at[k, :, c, t], b2_ss.at[k, 1, dt - 1], b2_rs.at[k, 1, dt - 1], y_peer(dt)) for dt in range(1, n_tp)]
        b3[k] = [send(ga.at[k, x, c], ga.at[k, x, c], b3_ss.at[k, 0, 0], b3_rs.at[k, 0, 0], partner), send(gb.at[k, :, c, t], gb.at[k, :, c, t], b3_ss.at[k, 1, 0], b3_rs.at[k, 1, 0], partner)]

    def third(k):
        for d in range(1, n_x):
            b2[k, 0][d - 1].wait_recv()
            xs = x_src(d)
            b3[k].append(send(ga.at[k, xs, c], ga.at[k, xs, c], b3_ss.at[k, 0, d], b3_rs.at[k, 0, d], partner))
            b2[k, 1][d - 1].wait_recv()
            ts = y_src(d)
            b3[k].append(send(gb.at[k, :, c, ts], gb.at[k, :, c, ts], b3_ss.at[k, 1, d], b3_rs.at[k, 1, d], partner))

    def gathered(k):
        for cp in b3[k]:
            cp.wait_recv()
        lo = k * k_cols
        for h, ref in ((0, ga), (1, gb)):
            h_s[:, lo + h * quarter:lo + (h + 1) * quarter] = ref[k, :, :, :, :, 0:quarter].astype(F32).reshape(n_tok, quarter).astype(BF16)

    for k in range(n_k - 1):
        first(k)
    logits = jnp.dot(h2, wr[...], preferred_element_type=F32)
    logits = jnp.where(mask_s[t] > 0.5, logits, -jnp.inf)
    ex = jnp.exp(logits - jnp.max(logits, axis=-1, keepdims=True))
    gb[n_k - 1, x, c, t, :, quarter:quarter + n_all] = (ex / jnp.sum(ex, axis=-1, keepdims=True)).astype(BF16)
    first(n_k - 1)
    for k in range(n_k):
        second(k)
    x1_sends = [send(x1_s.at[t], x1_s.at[t], x_ss.at[dt - 1], x_rs.at[dt - 1], y_peer(dt)) for dt in range(1, n_tp)]
    third(0)
    quad = 8
    wide = quad * ff

    def product(w, q, lo, hi):
        return lax.dot_general(h_s[:, lo:hi], w[q * quad:(q + 1) * quad, :, lo:hi].reshape(wide, hi - lo), NT, preferred_element_type=F32)

    lane = lax.broadcasted_iota(jnp.int32, (n_tok, 128), 1)
    for k in range(n_k):
        gathered(k)
        lo, hi = k * k_cols, (k + 1) * k_cols
        if k == n_k - 1:
            gates = gb[k, :, :, :, :, quarter:quarter + n_all].astype(F32).reshape(n_tok, n_all)
            gates = pltpu.roll(gates, lax.rem(n_all - e * n_exp, n_all), 1)
        for q in range(n_exp // quad):
            if k == 0:
                for p in range(q * quad // 2, (q + 1) * quad // 2):
                    wcopy(0, p).wait()
                    wcopy(1, p).wait()
            cols = slice(q * wide, (q + 1) * wide)
            gate_pre = product(wg, q, lo, hi)
            up_pre = product(wu, q, lo, hi)
            if k > 0:
                gate_pre = gate_pre + acc[0, :, cols]
                up_pre = up_pre + acc[1, :, cols]
            if k < n_k - 1:
                acc[0, :, cols] = gate_pre
                acc[1, :, cols] = up_pre
                if q == 0:
                    third(k + 1)
                continue
            y = (gate_pre * jax.nn.sigmoid(gate_pre) * up_pre).astype(BF16).astype(F32)
            g = [jnp.broadcast_to(gates[:, q * quad + i:q * quad + i + 1], (n_tok, 128)) for i in range(quad)]
            scale = []
            for lane0 in range(0, wide, 128):
                i = lane0 // ff
                edge = (i + 1) * ff - lane0
                scale.append(g[i] if edge >= 128 else jnp.where(lane < edge, g[i], g[i + 1]))
            act[:, cols] = (y * jnp.concatenate(scale, axis=-1)).astype(BF16)
    for p in range(n_pair):
        wcopy(2, p).wait()
    c0, c1, c2 = {}, {}, {}

    groups = []
    for j in range(n_cols):
        if starts[j] % 512 == 0:
            groups.append([])
        groups[-1].append(j)

    def down(i):
        lo, wide_n = starts[groups[i][0]], sum(widths[j] for j in groups[i])
        both = jnp.dot(act[...], wd[:, :, lo:lo + wide_n].reshape(n_exp * ff, wide_n), preferred_element_type=F32)
        for j in groups[i]:
            o32, c0_send, c0_recv = cbufs[j][0:3]
            o = both[:, starts[j] - lo:starts[j] - lo + widths[j]].reshape(n_x, 2, n_tp, rows, widths[j])
            o32[...] = o
            c0_send[...] = o.astype(BF16)
            c0[j] = send(c0_send.at[:, 1 - c], c0_recv, c0_ss.at[j], c0_rs.at[j], partner)

    def stage1(j):
        o32, _, c0_recv, c1_send, c1_own, c1_recv = cbufs[j][0:6]
        c0[j].wait_recv()
        total = o32[:, c] + c0_recv[...].astype(F32)
        c1_send[...] = total.astype(BF16)
        c1_own[...] = total
        c1[j] = [send(c1_send.at[x_dst(dx)], c1_recv.at[dx - 1], c1_ss.at[j, dx - 1], c1_rs.at[j, dx - 1], x_peer(dx)) for dx in range(1, n_x)]

    def stage2(j):
        c1_own, c1_recv, c2_buf = cbufs[j][4:7]
        total = c1_own[x]
        for dx in range(1, n_x):
            c1[j][dx - 1].wait_recv()
            total = total + c1_recv[dx - 1].astype(F32)
        c2_buf[t] = total.astype(BF16)
        c2[j] = [send(c2_buf.at[t], c2_buf.at[t], c2_ss.at[j, dt - 1], c2_rs.at[j, dt - 1], y_peer(dt)) for dt in range(1, n_tp)]

    outs = []

    def stage3(j):
        c2_buf = cbufs[j][6]
        if j == 0:
            for cp in x1_sends:
                cp.wait_recv()
        for cp in c2[j]:
            cp.wait_recv()
        cols = slice(starts[j], starts[j] + widths[j])
        total = c2_buf[0].astype(F32)
        for i in range(1, n_tp):
            total = total + c2_buf[i].astype(F32)
        outbuf[:, :, cols] = (x1_s[:, :, cols].astype(F32) + total).astype(BF16)
        where = (slice(None), slice(None), pl.ds(starts[j], widths[j]))
        cp = pltpu.make_async_copy(outbuf.at[where], out_hbm.at[where], sem_out.at[j])
        cp.start()
        outs.append(cp)

    plan = [(down, i, i) for i in range(len(groups))]
    for i, group in enumerate(groups):
        for n, j in enumerate(group):
            plan.append((stage1, j, i + 1.25 + 0.05 * n if i < len(groups) - 1 else i + 0.7 + 0.05 * n))
            plan.append((stage2, j, len(groups) - 0.4 + starts[j] / 400))
            plan.append((stage3, j, len(groups) + 2.0 + starts[j] / 400))
    for stage, j, _ in sorted(plan, key=lambda one: one[2]):
        stage(j)
    for cp in sent:
        cp.wait_send()
    for cp in outs:
        cp.wait()


def solution(mesh):
    n_ep = mesh.shape['ep']
    n_tp = mesh.shape['tp']
    n_x = n_ep // 2
    token_rows = P(('dp', 'ep'), None)
    token_vec = P(('dp', 'ep'))
    cache_spec = P(('dp', 'ep'), None, 'tp', None)
    expert_in = P('ep', None, 'tp')
    expert_down = P('ep', 'tp', None)
    hbm_spec = pl.BlockSpec(memory_space=pltpu.HBM)

    def device_step(hidden, seq_lens, rope_cos, rope_sin, ln1_scale, ln1_bias, w_qkv, b_qkv, w_out, b_out, k_cache, v_cache, ln2_scale, ln2_bias, w_router, expert_ids, w_gate, w_up, w_down):
        n_batch, d_model = hidden.shape
        _, s_max, n_kv, head = k_cache.shape
        n_q = w_qkv.shape[1] // head - 2
        rows = n_batch // n_tp
        n_qkv, group = 4, 8
        k3 = k_cache.reshape(n_batch, s_max, head)
        v3 = v_cache.reshape(n_batch, s_max, head)
        dma = pltpu.SemaphoreType.DMA
        ctx, k_out, v_out = pl.pallas_call(
            functools.partial(attention_kernel, n_qkv, group),
            out_shape=(jax.ShapeDtypeStruct((n_batch, n_q * head), BF16), jax.ShapeDtypeStruct(k3.shape, BF16), jax.ShapeDtypeStruct(v3.shape, BF16)),
            in_specs=[hbm_spec] * 10,
            out_specs=(hbm_spec,) * 3,
            scratch_shapes=[
                pltpu.SMEM(seq_lens.shape, jnp.int32),
                pltpu.VMEM(hidden.shape, BF16),
                pltpu.VMEM(rope_cos.shape, F32),
                pltpu.VMEM(rope_sin.shape, F32),
                pltpu.VMEM((d_model,), BF16),
                pltpu.VMEM((d_model,), BF16),
                pltpu.VMEM(b_qkv.shape, BF16),
                dma((7,)),
                pltpu.VMEM(w_qkv.shape, BF16),
                pltpu.VMEM(k3.shape, BF16),
                pltpu.VMEM(v3.shape, BF16),
                pltpu.VMEM((n_batch, n_q, head), F32),
                pltpu.VMEM((n_batch, n_q, head), F32),
                pltpu.VMEM((2, n_batch, head), F32),
                pltpu.VMEM((n_batch, n_q * head), BF16),
                dma((n_qkv,)), dma((n_batch // group,)), dma((n_batch // group,)), dma((n_batch // group,)), dma((n_batch // group,)),
            ],
            compiler_params=pltpu.CompilerParams(vmem_limit_bytes=63 * 1024 * 1024),
            name='attention',
        )(seq_lens, hidden, rope_cos, rope_sin, ln1_scale, ln1_bias, b_qkv, w_qkv, k3, v3)

        widths = (512, 512, 512, 256, 256)
        n_cols = len(widths)
        n_k, n_o = 2, 4
        quarter = d_model // (2 * n_k)
        wg = jnp.swapaxes(w_gate, 1, 2)
        wu = jnp.swapaxes(w_up, 1, 2)
        n_exp, ff, _ = wg.shape
        n_all = w_router.shape[1]
        n_tok = n_ep * n_batch
        ids_t = expert_ids.T
        V = pltpu.VMEM
        nx1, nt1 = n_x - 1, n_tp - 1
        assert n_tp == n_x
        out = pl.pallas_call(
            functools.partial(moe_kernel, n_tp, n_x, widths),
            out_shape=jax.ShapeDtypeStruct((n_tp, rows, d_model), BF16),
            in_specs=[hbm_spec] * 11,
            out_specs=hbm_spec,
            scratch_shapes=[
                V(ctx.shape, BF16), V((rows, d_model), BF16), V(ids_t.shape, jnp.int32),
                V((d_model,), BF16), V((d_model,), BF16), V((d_model,), BF16), V(w_out.shape, BF16), V(w_router.shape, BF16),
                V(wg.shape, BF16), V(wg.shape, BF16), V(wg.shape, BF16),
                V((n_tp, rows, n_all), F32),
                V((n_o, n_tp, rows, d_model // n_o), BF16),
                V((n_o, nt1, rows, d_model // n_o), BF16),
                V((n_tp, rows, d_model), BF16),
                V((n_k, n_x, 2, n_tp, rows, quarter), BF16),
                V((n_k, n_x, 2, n_tp, rows, quarter + n_all), BF16),
                V((n_tok, d_model), BF16),
                V((2, n_tok, n_exp * ff), F32),
                V((n_tok, n_exp * ff), BF16),
                V((n_tp, rows, d_model), BF16),
                [(V((n_x, 2, n_tp, rows, w), F32), V((n_x, 2, n_tp, rows, w), BF16), V((n_x, n_tp, rows, w), BF16),
                  V((n_x, n_tp, rows, w), BF16), V((n_x, n_tp, rows, w), F32), V((nx1, n_tp, rows, w), BF16), V((n_tp, n_tp, rows, w), BF16)) for w in widths],
                dma((7,)), dma((n_o,)), dma((3, n_exp // 2)),
                dma((n_o, nt1)), dma((n_o, nt1)),
                dma((n_k, 2, nx1)), dma((n_k, 2, nx1)), dma((n_k, 2, nx1)), dma((n_k, 2, nx1)), dma((n_k, 2, n_x)), dma((n_k, 2, n_x)),
                dma((nt1,)), dma((nt1,)),
                dma((n_cols,)), dma((n_cols,)), dma((n_cols, nx1)), dma((n_cols, nx1)), dma((n_cols, nt1)), dma((n_cols, nt1)),
                dma((n_cols,)),
            ],
            compiler_params=pltpu.CompilerParams(vmem_limit_bytes=63 * 1024 * 1024, collective_id=0, has_side_effects=True),
            name='moe',
        )(ctx, hidden.reshape(n_tp, rows, d_model), ids_t, b_out, ln2_scale, ln2_bias, w_out, w_router, wg, wu, w_down)
        return out.reshape(n_batch, d_model), k_out.reshape(k_cache.shape), v_out.reshape(v_cache.shape)

    in_specs = (token_rows, token_vec, token_rows, token_rows, P(), P(), P(None, 'tp'), P('tp'), P('tp', None), P(), cache_spec, cache_spec, P(), P(), P(), token_rows, expert_in, expert_in, expert_down)
    return jax.shard_map(device_step, mesh=mesh, in_specs=in_specs, out_specs=(token_rows, cache_spec, cache_spec), check_vma=False)
```
